32 devices in a mesh: lat: 4 (over y, core), lon: 8 (over z, x).
Axes of the slice: x: 2, y: 2, z: 4, core: 2. Of those that a mesh axis runs over, the one named last changes fastest.
Arguments:
- layer_temp: float32 [64, 35, 1024], P('lat', None, 'lon'), may hold values from -20 to -2
- ice_depth_per_class: float32 [64, 5, 1024], P('lat', None, 'lon'), may hold values from 0.5 to 3
- ice_area: float32 [64, 5, 1024], P('lat', None, 'lon'), may hold values from 0.05 to 0.2
- surf_temp: float32 [64, 1024], P('lat', 'lon'), may hold values from -30 to -2
- seawater_thermal_input: float32 [64, 1024], P('lat', 'lon'), may hold values from 0 to 0.3
- velocity: float32 [2, 64, 1024], P(None, 'lat', 'lon'), may hold values from -1.2 to 1.2
- stress: float32 [3, 64, 1024], P(None, 'lat', 'lon'), may hold values from -3 to 3
- wind_stress: float32 [2, 64, 1024], P(None, 'lat', 'lon'), may hold values from -1.8 to 1.8
- current: float32 [2, 64, 1024], P(None, 'lat', 'lon'), may hold values from -1.8 to 1.8
- land_mask: int32 [64, 1024], P('lat', 'lon'), may hold values 0 or 1
- ice_mask: int32 [8, 64], P('lon', 'lat'), may hold values from 0 to 1, as said below
- band_index: int32 [64], P('lat'), may hold values from 0 to 15, as said below
Outputs:
- temp_after: float32 [64, 35, 1024], P('lat', None, 'lon')
- thick_after: float32 [64, 5, 1024], P('lat', None, 'lon')
- velocity_after: float32 [2, 64, 1024], P(None, 'lat', 'lon')
- stress_after: float32 [3, 64, 1024], P(None, 'lat', 'lon')
- zonal_volume: float32 [16], P('lat')
The draws below stay inside these ranges and needn't reach their ends.
Inputs may be any that keep to these rules, and one draw needn't show every extreme that they name: `ice_mask`: for each lat index, the strips of all devices with that index include at most 56 ice-covered strips and more than (6) times the number of lon devices; among these devices one has all its 16 strips ice-covered. `band_index`: every band holds 1 to 7 rows, which lie next to one another; one band holds exactly 7.
All inputs are finite; a program needn't handle non-finite values. No bound on the sum of `land_mask` on one device may be relied on, other than what follows from the above.
Results may differ from the reference program's by a relative error of at most 0.00002.
Values sent between devices are 32-bit elements; how exact they have to be, the bound alone decides.
A program may use at most 64 MiB of HBM per device.

```python
import math
import jax
import jax.numpy as jnp
from jax import lax

DEPTH_CLASSES = 5
VERTICAL_LEVELS = 7
ROWS_DEV = 16
COLS_DEV = 128
SUBCYCLES = 3
SWEEPS = 2
ICE_DEV = 7
GRID_ROWS = 64
GRID_COLS = 1024
BANDS = 16
N_LAT = 4
N_LON = 8


def ice_row_group(group_key):
    count_key, full_key, shuffle_key = jax.random.split(group_key, 3)
    strip_total = N_LON * ROWS_DEV
    ice_total = N_LON * (ICE_DEV - 1) + jax.random.randint(count_key, (), 1, N_LON + 1)
    full_device = jax.random.randint(full_key, (), 0, N_LON)
    shuffled = jax.random.permutation(shuffle_key, strip_total)
    owner_lon = jnp.arange(strip_total, dtype=jnp.int32) // ROWS_DEV
    priority = jnp.where(owner_lon == full_device, shuffled - strip_total, shuffled)
    position = jnp.argsort(jnp.argsort(priority, stable=True), stable=True)
    return (position < ice_total).astype(jnp.int32).reshape(N_LON, ROWS_DEV)


def draw_ice_mask(key, part):
    row_keys = jax.random.split(jax.random.fold_in(key, 7), N_LAT)
    grouped = jax.vmap(ice_row_group)(row_keys)
    return jnp.transpose(grouped, (1, 0, 2)).reshape(N_LON, N_LAT * ROWS_DEV)


def draw_band_index(key, part):
    shift_key, pick_key, pair_key = jax.random.split(jax.random.fold_in(key, 11), 3)
    base_rows = ROWS_DEV // 4
    pair_count = BANDS // 2
    moved = jax.random.randint(shift_key, (pair_count,), -(base_rows - 1), base_rows)
    chosen_pair = jax.random.randint(pick_key, (), 0, pair_count)
    moved = jnp.where(jnp.arange(pair_count, dtype=jnp.int32) == chosen_pair, base_rows - 1, moved)
    shuffled = jax.random.permutation(pair_key, BANDS).astype(jnp.int32)
    place = jnp.argsort(shuffled, stable=True).astype(jnp.int32)
    pair_of_band = place // 2
    side = place % 2
    band_rows = (base_rows + moved[pair_of_band] * (1 - 2 * side)).astype(jnp.int32)
    band_ends = jnp.cumsum(band_rows)
    row_ids = jnp.arange(GRID_ROWS, dtype=jnp.int32)
    upward = jnp.sum((band_ends[None, :] <= row_ids[:, None]).astype(jnp.int32), axis=1)
    return ((upward + BANDS // 2) % BANDS).astype(jnp.int32)


def place_ends(entries, key, low, top_value):
    shape = entries.shape
    index_at = [jax.random.randint(jax.random.fold_in(key, axis), (), 0, shape[axis]) for axis in range(len(shape))]
    entries = entries.at[tuple(index_at)].set(low)
    longest = shape.index(max(shape))
    index_at[longest] = (index_at[longest] + 1) % shape[longest]
    return entries.at[tuple(index_at)].set(top_value)


def shard_levels(stream_key, dims, cuts, least, largest):
    def one(axis_at, parts):
        steps = jax.random.uniform(jax.random.fold_in(jax.random.fold_in(stream_key, 6), axis_at), (parts,), jnp.float32, least / len(cuts), largest / len(cuts))
        return jnp.repeat(jnp.exp(steps), dims[axis_at] // parts).reshape((-1,) + (1,) * (len(dims) - axis_at - 1))

    level = one(*cuts[0])
    for cut in cuts[1:]:
        level = level * one(*cut)
    return level


def gaussian(rng, shape, spread, reach, cuts=(), kind=jnp.bfloat16):
    result = spread * jax.random.normal(rng, shape, jnp.float32)
    if cuts:
        result = result * shard_levels(rng, shape, cuts, -0.22, 0.18)
    return jnp.clip(result, -reach, reach).astype(kind)


def setup_inputs(seed: int = 0) -> dict:
    streams_of = jax.random.split(jax.random.key(seed), 13)
    layer_temp = jnp.clip(-20.0 + 18.0 * jax.random.uniform(streams_of[0], (GRID_ROWS, DEPTH_CLASSES * VERTICAL_LEVELS, GRID_COLS), jnp.float32) ** shard_levels(streams_of[0], (GRID_ROWS, DEPTH_CLASSES * VERTICAL_LEVELS, GRID_COLS), ((0, 4), (2, 8)), -0.2, 0.2), -20.0, -2.0)
    ice_depth_per_class = jnp.clip(jnp.exp(math.log(3.0) - 1.7917595 * jax.random.uniform(streams_of[1], (GRID_ROWS, DEPTH_CLASSES, GRID_COLS), jnp.float32) ** shard_levels(streams_of[1], (GRID_ROWS, DEPTH_CLASSES, GRID_COLS), ((0, 4), (2, 8)), -0.2, 0.2)), 0.5, 3.0)
    ice_area = jnp.clip(jnp.exp(math.log(0.2) - 1.3862944 * jax.random.uniform(streams_of[2], (GRID_ROWS, DEPTH_CLASSES, GRID_COLS), jnp.float32) ** shard_levels(streams_of[2], (GRID_ROWS, DEPTH_CLASSES, GRID_COLS), ((0, 4), (2, 8)), -0.2, 0.2)), 0.05, 0.2)
    surf_temp = jnp.clip(-30.0 + 28.0 * jax.random.uniform(streams_of[3], (GRID_ROWS, GRID_COLS), jnp.float32) ** shard_levels(streams_of[3], (GRID_ROWS, GRID_COLS), ((0, 4), (1, 8)), -0.2, 0.2), -30.0, -2.0)
    seawater_thermal_input = jnp.clip(0.3 * jax.random.uniform(streams_of[4], (GRID_ROWS, GRID_COLS), jnp.float32) ** shard_levels(streams_of[4], (GRID_ROWS, GRID_COLS), ((0, 4), (1, 8)), -0.2, 0.2), 0.0, 0.3)
    velocity = gaussian(streams_of[5], (2, GRID_ROWS, GRID_COLS), 0.2, 1.2, ((1, 4), (2, 8)), jnp.float32)
    stress = gaussian(streams_of[6], (3, GRID_ROWS, GRID_COLS), 0.5, 3.0, ((1, 4), (2, 8)), jnp.float32)
    wind_stress = gaussian(streams_of[7], (2, GRID_ROWS, GRID_COLS), 0.3, 1.8, ((1, 4), (2, 8)), jnp.float32)
    current = gaussian(streams_of[8], (2, GRID_ROWS, GRID_COLS), 0.3, 1.8, ((1, 4), (2, 8)), jnp.float32)
    land_mask = place_ends((jax.random.randint(streams_of[9], (GRID_ROWS, GRID_COLS), 0, 10) < 9).astype(jnp.int32), jax.random.fold_in(streams_of[9], 1), 0, 1)
    ice_mask = draw_ice_mask(jax.random.fold_in(streams_of[12], 71), 0)
    band_index = draw_band_index(jax.random.fold_in(streams_of[12], 71), 0)
    return dict(layer_temp=layer_temp, ice_depth_per_class=ice_depth_per_class, ice_area=ice_area, surf_temp=surf_temp, seawater_thermal_input=seawater_thermal_input, velocity=velocity, stress=stress, wind_stress=wind_stress, current=current, land_mask=land_mask, ice_mask=ice_mask, band_index=band_index)


FREEZE_POINT = -1.8
BASE_CONDUCT = 2.03
SALT_CONDUCT = 0.416
CONDUCT_SCALE = 1.0
GROWTH_RATE = 0.02
STRENGTH_SCALE = 1.0
STRENGTH_DECAY = 5.0
ELLIPSE_SQUARE = 4.0
STRAIN_FLOOR = 0.0025
STRESS_RELAX = 0.5
MOMENTUM_STEP = 0.5
WATER_DRAG = 1.0

def update_vertical_cell(thermal_state_levels, ice_depth_per_class, upper_interface_state, seawater_thermal_input):
    first_extent = thermal_state_levels.shape[:-2]
    vertical_cell_group = thermal_state_levels.shape[-1]
    vertical_levels_state = thermal_state_levels.reshape(first_extent + (DEPTH_CLASSES, VERTICAL_LEVELS, vertical_cell_group))
    before = [vertical_levels_state[..., layer_at, :] for layer_at in range(VERTICAL_LEVELS)]
    surface_row = upper_interface_state[..., None, :]
    scaled = CONDUCT_SCALE / (ice_depth_per_class * ice_depth_per_class)
    repeated_pass = before
    for picard_turn in range(SWEEPS):
        conductance = [BASE_CONDUCT + SALT_CONDUCT / guessed for guessed in repeated_pass]
        couplings = [scaled * conductance[0]]
        for layer_at in range(1, VERTICAL_LEVELS):
            couplings.append(scaled * 0.5 * (conductance[layer_at - 1] + conductance[layer_at]))
        couplings.append(scaled * conductance[VERTICAL_LEVELS - 1])
        upper_ratio = []
        eliminated = []
        for layer_at in range(VERTICAL_LEVELS):
            source_term = before[layer_at]
            divisor = 1.0 + couplings[layer_at] + couplings[layer_at + 1]
            if layer_at == 0:
                source_term = source_term + couplings[0] * surface_row
            else:
                divisor = divisor - couplings[layer_at] * upper_ratio[layer_at - 1]
                source_term = source_term + couplings[layer_at] * eliminated[layer_at - 1]
            if layer_at == VERTICAL_LEVELS - 1:
                source_term = source_term + couplings[VERTICAL_LEVELS] * FREEZE_POINT
            upper_ratio.append(couplings[layer_at + 1] / divisor)
            eliminated.append(source_term / divisor)
        solved = list(eliminated)
        for layer_at in range(VERTICAL_LEVELS - 2, -1, -1):
            solved[layer_at] = eliminated[layer_at] + upper_ratio[layer_at] * solved[layer_at + 1]
        repeated_pass = solved
    bottom = repeated_pass[VERTICAL_LEVELS - 1]
    regrown = ice_depth_per_class + GROWTH_RATE * (BASE_CONDUCT + SALT_CONDUCT / bottom) * (FREEZE_POINT - bottom) / ice_depth_per_class - seawater_thermal_input[..., None, :]
    updated_vertical_cells = jnp.stack(repeated_pass, axis=-2).reshape(thermal_state_levels.shape)
    return (updated_vertical_cells, regrown)

def pad_rim(field, margin):
    wrapped = jnp.concatenate([field[..., -margin:], field, field[..., :margin]], axis=-1)
    spacing = [(0, 0)] * (field.ndim - 2) + [(margin, margin), (0, 0)]
    return jnp.pad(wrapped, spacing)

def stress_update(zonal_field, meridional_field, previous, strength):
    zonal_east = (zonal_field[1:-1, 2:] - zonal_field[1:-1, :-2]) * 0.5
    zonal_north = (zonal_field[2:, 1:-1] - zonal_field[:-2, 1:-1]) * 0.5
    meridional_east = (meridional_field[1:-1, 2:] - meridional_field[1:-1, :-2]) * 0.5
    meridional_north = (meridional_field[2:, 1:-1] - meridional_field[:-2, 1:-1]) * 0.5
    divergence = zonal_east + meridional_north
    tension = zonal_east - meridional_north
    shearing = zonal_north + meridional_east
    deformation = jnp.sqrt(divergence * divergence + (tension * tension + shearing * shearing) / ELLIPSE_SQUARE + STRAIN_FLOOR)
    viscous = strength / deformation
    bulk_new = (previous[0] + STRESS_RELAX * viscous * (divergence - deformation)) / (1.0 + STRESS_RELAX)
    tension_new = (previous[1] + STRESS_RELAX * viscous * tension / ELLIPSE_SQUARE) / (1.0 + STRESS_RELAX)
    shear_new = (previous[2] + STRESS_RELAX * viscous * shearing / (2.0 * ELLIPSE_SQUARE)) / (1.0 + STRESS_RELAX)
    return jnp.stack([bulk_new, tension_new, shear_new])

def force_update(padded, velocity, ice_mass, wind_stress, current, wet_cells):
    normal_east = 0.5 * (padded[0] + padded[1])
    normal_north = 0.5 * (padded[0] - padded[1])
    shear_stress = padded[2]
    push_east = (normal_east[1:-1, 2:] - normal_east[1:-1, :-2]) * 0.5 + (shear_stress[2:, 1:-1] - shear_stress[:-2, 1:-1]) * 0.5
    push_north = (shear_stress[1:-1, 2:] - shear_stress[1:-1, :-2]) * 0.5 + (normal_north[2:, 1:-1] - normal_north[:-2, 1:-1]) * 0.5
    pushes = jnp.stack([push_east, push_north])
    moved = velocity + MOMENTUM_STEP * (pushes / ice_mass + wind_stress + WATER_DRAG * current)
    return wet_cells * moved / (1.0 + MOMENTUM_STEP * WATER_DRAG)

def one_block(pieces):
    return update_vertical_cell(pieces[0], pieces[1], pieces[2], pieces[3])

def reference(layer_temp, ice_depth_per_class, ice_area, surf_temp, seawater_thermal_input, velocity, stress, wind_stress, current, land_mask, ice_mask, band_index):
    strip_ice = jnp.repeat(jnp.transpose(ice_mask), COLS_DEV, axis=1) == 1
    blocks = (layer_temp.reshape(N_LAT, ROWS_DEV, DEPTH_CLASSES * VERTICAL_LEVELS, GRID_COLS), ice_depth_per_class.reshape(N_LAT, ROWS_DEV, DEPTH_CLASSES, GRID_COLS), surf_temp.reshape(N_LAT, ROWS_DEV, GRID_COLS), seawater_thermal_input.reshape(N_LAT, ROWS_DEV, GRID_COLS))
    stepped_temp, stepped_thick = lax.map(one_block, blocks)
    stepped_temp = stepped_temp.reshape(layer_temp.shape)
    stepped_thick = stepped_thick.reshape(ice_depth_per_class.shape)
    temp_after = jnp.where(strip_ice[:, None, :], stepped_temp, layer_temp)
    thick_after = jnp.where(strip_ice[:, None, :], stepped_thick, ice_depth_per_class)
    volume_start = lax.optimization_barrier(jnp.sum(ice_area * ice_depth_per_class, axis=1))
    coverage = lax.optimization_barrier(jnp.sum(ice_area, axis=1))
    strength = STRENGTH_SCALE * volume_start * jnp.exp(-STRENGTH_DECAY * (1.0 - coverage))
    ice_mass = 1.0 + volume_start
    wet_cells = land_mask.astype(jnp.float32)
    moving = velocity
    stresses = stress
    for subcycle in range(SUBCYCLES):
        padded_velocity = pad_rim(moving, 1)
        stresses = stress_update(padded_velocity[0], padded_velocity[1], stresses, strength)
        moving = force_update(pad_rim(stresses, 1), moving, ice_mass, wind_stress, current, wet_cells)
    volume_after = lax.optimization_barrier(jnp.sum(ice_area * thick_after, axis=1))
    row_total = lax.optimization_barrier(jnp.sum(volume_after, axis=1))
    members = (band_index[:, None] == jnp.arange(BANDS, dtype=jnp.int32)[None, :]).astype(jnp.float32)
    band_sum = lax.optimization_barrier(jnp.sum(members * row_total[:, None], axis=0))
    band_cells = lax.optimization_barrier(jnp.sum(members, axis=0)) * GRID_COLS
    zonal_volume = band_sum / band_cells
    return (temp_after, thick_after, moving, stresses, zonal_volume)
```

```python
import functools

import jax
import jax.numpy as jnp
from jax import lax
from jax.experimental import pallas as pl
from jax.experimental.pallas import tpu as pltpu
from jax.sharding import PartitionSpec as P

DEPTH_CLASSES = 5
VERTICAL_LEVELS = 7
SUBCYCLES = 3
SWEEPS = 2
BANDS_DEV = 4

FREEZE_POINT = -1.8
BASE_CONDUCT = 2.03
SALT_CONDUCT = 0.416
GROWTH_RATE = 0.02
STRENGTH_DECAY = 5.0
ELLIPSE_SQUARE = 4.0
STRAIN_FLOOR = 0.0025
STRESS_RELAX = 0.5
MOMENTUM_STEP = 0.5
WATER_DRAG = 1.0

HALO = 2 * SUBCYCLES
EDGE = 8
FIELDS = 10
FIRST_DYNAMIC = DEPTH_CLASSES * (VERTICAL_LEVELS + 2) + 2
DYNAMIC = 9
UNROLLED = 64

MESH = pl.DeviceIdType.MESH


def step_columns(temps, depth, surface, seawater):
    inverse = 1.0 / depth
    scaled = inverse * inverse
    half = 0.5 * scaled
    guess = temps
    for turn in range(SWEEPS):
        conduct = [BASE_CONDUCT + SALT_CONDUCT / g for g in guess]
        coupling = [scaled * conduct[0]]
        for k in range(1, VERTICAL_LEVELS):
            coupling.append(half * (conduct[k - 1] + conduct[k]))
        coupling.append(scaled * conduct[-1])
        ratio, done = [], []
        for k in range(VERTICAL_LEVELS):
            source = temps[k]
            divisor = 1.0 + coupling[k] + coupling[k + 1]
            if k == 0:
                source = source + coupling[0] * surface
            else:
                divisor = divisor - coupling[k] * ratio[k - 1]
                source = source + coupling[k] * done[k - 1]
            if k == VERTICAL_LEVELS - 1:
                source = source + coupling[k + 1] * FREEZE_POINT
            scale = 1.0 / divisor
            if k < VERTICAL_LEVELS - 1:
                ratio.append(coupling[k + 1] * scale)
            done.append(source * scale)
        solved = list(done)
        for k in range(VERTICAL_LEVELS - 2, -1, -1):
            solved[k] = done[k] + ratio[k] * solved[k + 1]
        guess = solved
    bottom = guess[-1]
    thick = (
        depth
        + GROWTH_RATE * (BASE_CONDUCT + SALT_CONDUCT / bottom) * (FREEZE_POINT - bottom) * inverse
        - seawater
    )
    return guess, thick


def subcycle(u, v, s1, s2, s12, strength, keep, push_scale, force_x, force_y):
    rows, cols = u.shape

    def dx(f):
        return pltpu.roll(f, cols - 1, 1) - pltpu.roll(f, 1, 1)

    def dy(f):
        return pltpu.roll(f, rows - 1, 0) - pltpu.roll(f, 1, 0)

    ux, vy, uy, vx = dx(u), dy(v), dy(u), dx(v)
    divergence = 0.5 * (ux + vy)
    tension = 0.5 * (ux - vy)
    shearing = 0.5 * (uy + vx)
    deformation = jnp.sqrt(
        divergence * divergence
        + (tension * tension + shearing * shearing) * (1.0 / ELLIPSE_SQUARE)
        + STRAIN_FLOOR
    )
    relax = 1.0 / (1.0 + STRESS_RELAX)
    viscous = (STRESS_RELAX * relax) * strength / deformation
    s1 = relax * s1 + viscous * (divergence - deformation)
    s2 = relax * s2 + viscous * tension * (1.0 / ELLIPSE_SQUARE)
    s12 = relax * s12 + viscous * shearing * (0.5 / ELLIPSE_SQUARE)
    push_x = dx(0.5 * (s1 + s2)) + dy(s12)
    push_y = dx(s12) + dy(0.5 * (s1 - s2))
    u = keep * u + push_scale * push_x + force_x
    v = keep * v + push_scale * push_y + force_y
    return u, v, s1, s2, s12


def as_column(row, rows):
    shape = (rows, rows)
    pick = lax.broadcasted_iota(jnp.int32, shape, 0) == lax.broadcasted_iota(jnp.int32, shape, 1)
    wide = jnp.broadcast_to(row.astype(jnp.float32), shape)
    return jnp.sum(jnp.where(pick, wide, 0.0), axis=1, keepdims=True)


def kernel(n_lat, n_lon, *refs):
    inputs, outputs, scratch = refs[:12], refs[12:17], refs[17:]
    temp_out, thick_out, vel_out, stress_out, zonal_out = outputs
    (held, land_in, ice_in, band_in, own, packed, edges, sides, parts) = scratch[:9]
    (in_sem, send_sem, recv_sem) = scratch[9:]
    rows, cols = land_in.shape
    devices = n_lat * n_lon
    lat, lon = lax.axis_index("lat"), lax.axis_index("lon")
    lats = [lax.rem(lat + d, n_lat) for d in range(n_lat)]
    lons = [lax.rem(lon + d, n_lon) for d in range(n_lon)]
    south, north, east, west = lats[1], lats[-1], lons[1], lons[-1]
    me = lon * n_lat + lat

    places = []
    first = 0
    for i in range(9):
        planes = 1 if len(inputs[i].shape) == 2 else inputs[i].shape[0]
        places.append(held.at[first] if len(inputs[i].shape) == 2 else held.at[pl.ds(first, planes)])
        first += planes
    targets = places + [land_in, ice_in, band_in]
    group = (0,) * 5 + (1,) * 4 + (2, 3, 4)

    def load(i):
        return pltpu.make_async_copy(inputs[i], targets[i], in_sem.at[group[i]])

    for i in (11, 10, 1, 2, 3, 4, 0, 5, 6, 7, 8, 9):
        load(i).start()

    def everyone(visit):
        if devices <= UNROLLED:
            for g in lons[1:] + lons[:1]:
                for a in lats:
                    if not (g is lons[0] and a is lats[0]):
                        visit((a, g))
        else:
            def step(d, carry):
                other = lax.rem(me + 1 + d, devices)
                visit((lax.rem(other, n_lat), other // n_lat))
                return carry

            lax.fori_loop(0, devices - 1, step, 0)

    barrier = pltpu.get_barrier_semaphore()
    everyone(
        lambda device: pl.semaphore_signal(
            barrier, inc=1, device_id=device, device_id_type=MESH
        )
    )

    load(11).wait()
    load(10).wait()
    icy = as_column(ice_in[...], rows) == 1.0
    width = parts.shape[-1]
    band = as_column(band_in[...], rows).astype(jnp.int32)
    slot = lax.broadcasted_iota(jnp.int32, (rows, width), 1)
    member = band == slot
    counted = jnp.where(band + width // 2 == slot, float(cols), 0.0)

    column = held.at[pl.ds(0, FIRST_DYNAMIC)]
    pltpu.make_async_copy(column, column, in_sem.at[0]).wait()
    temp_in, depth_in, area_in, surf_in, sea_in = places[:5]
    vel_in, stress_in, wind_in, current_in = places[5:]
    surface, seawater = surf_in[...], sea_in[...]
    after = jnp.zeros((rows, cols), jnp.float32)
    for c in range(DEPTH_CLASSES):
        first = c * VERTICAL_LEVELS
        temps = [temp_in[first + k] for k in range(VERTICAL_LEVELS)]
        depth = depth_in[c]
        stepped, thick = step_columns(temps, depth, surface, seawater)
        thick = jnp.where(icy, thick, depth)
        for k in range(VERTICAL_LEVELS):
            temp_out[first + k] = jnp.where(icy, stepped[k], temps[k])
        thick_out[c] = thick
        after = after + area_in[c] * thick
    total = jnp.sum(after, axis=1, keepdims=True)
    parts[pl.ds(me, 1)] = jnp.sum(jnp.where(member, total, counted), axis=0, keepdims=True)

    pl.semaphore_wait(barrier, devices - 1)

    def send_part(device):
        pltpu.make_async_remote_copy(
            src_ref=parts.at[pl.ds(me, 1)],
            dst_ref=parts.at[pl.ds(me, 1)],
            send_sem=send_sem.at[0],
            recv_sem=recv_sem.at[0],
            device_id=device,
            device_id_type=MESH,
        ).start()

    everyone(send_part)

    dynamic = held.at[pl.ds(FIRST_DYNAMIC, DYNAMIC)]
    pltpu.make_async_copy(dynamic, dynamic, in_sem.at[1]).wait()
    load(9).wait()
    volume = area_in[0] * depth_in[0]
    coverage = area_in[0]
    for c in range(1, DEPTH_CLASSES):
        volume = volume + area_in[c] * depth_in[c]
        coverage = coverage + area_in[c]
    strength = volume * jnp.exp(-STRENGTH_DECAY * (1.0 - coverage))
    drag = 1.0 / (1.0 + MOMENTUM_STEP * WATER_DRAG)
    keep = land_in[...].astype(jnp.float32) * drag
    forced = MOMENTUM_STEP * keep
    push_scale = 0.5 * forced / (1.0 + volume)
    fields = [vel_in[0], vel_in[1], stress_in[0], stress_in[1], stress_in[2], strength, keep]
    fields += [push_scale]
    fields += [forced * (wind_in[i] + WATER_DRAG * current_in[i]) for i in range(2)]
    lane = lax.broadcasted_iota(jnp.int32, (rows, cols), 1)
    pack = jnp.zeros((rows, cols), jnp.float32)
    for f in range(FIELDS):
        first = 2 * HALO * f
        turned = pltpu.roll(fields[f], (first + HALO) % cols, 1)
        pack = jnp.where((lane >= first) & (lane < first + 2 * HALO), turned, pack)
    packed[...] = pack
    for f in range(FIELDS):
        own[f] = fields[f]

    tail, head = pl.ds(rows - EDGE, EDGE), pl.ds(0, EDGE)
    above, middle, below = pl.ds(0, EDGE), pl.ds(EDGE, rows), pl.ds(EDGE + rows, EDGE)
    plan = (
        (packed.at[tail], sides.at[0, above], (south, east), 1),
        (packed.at[tail], sides.at[1, above], (south, west), 1),
        (packed.at[head], sides.at[0, below], (north, east), 1),
        (packed.at[head], sides.at[1, below], (north, west), 1),
        (packed, sides.at[0, middle], (lat, east), 1),
        (packed, sides.at[1, middle], (lat, west), 1),
        (own.at[:, tail], edges.at[0], (south, lon), 2),
        (own.at[:, head], edges.at[1], (north, lon), 2),
    )
    for source, target, device, arrival in plan:
        pltpu.make_async_remote_copy(
            src_ref=source,
            dst_ref=target,
            send_sem=send_sem.at[1],
            recv_sem=recv_sem.at[arrival],
            device_id=device,
            device_id_type=MESH,
        ).start()

    pltpu.make_async_copy(edges, edges, recv_sem.at[2]).wait()
    pltpu.make_async_copy(sides, sides, recv_sem.at[1]).wait()
    tall = rows + 2 * EDGE
    place = lax.broadcasted_iota(jnp.int32, (tall, cols), 1)
    merged = jnp.where(lax.rem(place, 2 * HALO) < HALO, sides[0], sides[1])
    low = jnp.where(lat == 0, EDGE, 0)
    high = jnp.where(lat == n_lat - 1, EDGE + rows, tall)
    row_id = lax.broadcasted_iota(jnp.int32, (tall, 2 * cols), 0)
    inside = (row_id >= low) & (row_id < high)
    state = []
    for f in range(FIELDS):
        centre = jnp.concatenate([edges[0, f], own[f], edges[1, f]], axis=0)
        beside = pltpu.roll(merged, (cols - 2 * HALO * f - HALO) % cols, 1)
        state.append(jnp.where(inside, jnp.concatenate([centre, beside], axis=1), 0.0))
    moving, fixed = state[:5], state[5:]
    for turn in range(SUBCYCLES):
        moving = subcycle(*moving, *fixed)
    for i in range(2):
        vel_out[i] = moving[i][EDGE : EDGE + rows, :cols]
    for i in range(3):
        stress_out[i] = moving[2 + i][EDGE : EDGE + rows, :cols]

    sent = held.at[pl.ds(0, (4 * EDGE + 2 * rows + 2 * FIELDS * EDGE) // rows)]
    pltpu.make_async_copy(sent, sent, send_sem.at[1]).wait()
    others = parts.at[pl.ds(0, devices - 1)]
    pltpu.make_async_copy(others, others, send_sem.at[0]).wait()
    pltpu.make_async_copy(others, others, recv_sem.at[0]).wait()
    whole = jnp.sum(parts[...], axis=0, keepdims=True)
    whole = pltpu.roll(whole, lax.rem(width - lat * BANDS_DEV, width), 1)
    cells = pltpu.roll(whole, width // 2, 1)
    mean = whole / jnp.maximum(cells, 1.0)
    zonal_out[...] = mean[:, :BANDS_DEV]


def put_out(*refs):
    sem = refs[10]
    copies = [pltpu.make_async_copy(refs[i], refs[5 + i], sem.at[i]) for i in range(5)]
    for copy in copies:
        copy.start()
    for copy in copies:
        copy.wait()


def local(n_lat, n_lon, *args):
    args = list(args)
    args[:3] = [jnp.transpose(a, (1, 0, 2)) for a in args[:3]]
    args[11] = args[11].reshape(1, -1)
    rows, cols = args[3].shape
    width = -(-2 * BANDS_DEV * n_lat // cols) * cols
    tall = rows + 2 * EDGE
    f32 = jnp.float32
    vmem = pl.BlockSpec(memory_space=pltpu.VMEM)
    shapes = [args[i].shape for i in (0, 1, 5, 6)] + [(1, BANDS_DEV)]
    dma = pltpu.SemaphoreType.DMA
    results = pl.pallas_call(
        functools.partial(kernel, n_lat, n_lon),
        out_shape=[pltpu.VMEM(shape, f32) for shape in shapes],
        in_specs=[pl.BlockSpec(memory_space=pl.ANY)] * 12,
        out_specs=[vmem] * 5,
        scratch_shapes=[
            pltpu.VMEM((FIRST_DYNAMIC + DYNAMIC, rows, cols), f32),
            *[pltpu.VMEM(a.shape, a.dtype) for a in args[9:]],
            pltpu.VMEM((FIELDS, rows, cols), f32),
            pltpu.VMEM((rows, cols), f32),
            pltpu.VMEM((2, FIELDS, EDGE, cols), f32),
            pltpu.VMEM((2, tall, cols), f32),
            pltpu.VMEM((n_lat * n_lon, width), f32),
            dma((5,)),
            dma((2,)),
            dma((3,)),
        ],
        compiler_params=pltpu.CompilerParams(collective_id=0, has_side_effects=True),
        name="ice_step",
    )(*args)
    temp, thick, vel, stress, zonal = pl.pallas_call(
        put_out,
        out_shape=[jax.ShapeDtypeStruct(shape, f32) for shape in shapes],
        in_specs=[vmem] * 5,
        out_specs=[pl.BlockSpec(memory_space=pl.ANY)] * 5,
        scratch_shapes=[dma((5,))],
        name="put_out",
    )(*[pltpu.with_memory_space_constraint(r, pltpu.VMEM) for r in results])
    temp, thick = [jnp.transpose(a, (1, 0, 2)) for a in (temp, thick)]
    return (temp, thick, vel, stress, zonal.reshape(BANDS_DEV))


def solution(mesh):
    shape = dict(mesh.shape)
    return jax.shard_map(
        functools.partial(local, shape["lat"], shape["lon"]),
        mesh=mesh,
        in_specs=(
            P("lat", None, "lon"),
            P("lat", None, "lon"),
            P("lat", None, "lon"),
            P("lat", "lon"),
            P("lat", "lon"),
            P(None, "lat", "lon"),
            P(None, "lat", "lon"),
            P(None, "lat", "lon"),
            P(None, "lat", "lon"),
            P("lat", "lon"),
            P("lon", "lat"),
            P("lat"),
        ),
        out_specs=(
            P("lat", None, "lon"),
            P("lat", None, "lon"),
            P(None, "lat", "lon"),
            P(None, "lat", "lon"),
            P("lat"),
        ),
        check_vma=False,
    )
```

```python
import functools

import jax
import jax.numpy as jnp
from jax import lax
from jax.experimental import pallas as pl
from jax.experimental.pallas import tpu as pltpu
from jax.sharding import PartitionSpec as P

DEPTH_CLASSES = 5
VERTICAL_LEVELS = 7
SUBCYCLES = 3
SWEEPS = 2
BANDS_DEV = 4

FREEZE_POINT = -1.8
BASE_CONDUCT = 2.03
SALT_CONDUCT = 0.416
GROWTH_RATE = 0.02
STRENGTH_DECAY = 5.0
ELLIPSE_SQUARE = 4.0
STRAIN_FLOOR = 0.0025
STRESS_RELAX = 0.5
MOMENTUM_STEP = 0.5
WATER_DRAG = 1.0

HALO = 2 * SUBCYCLES
EDGE = 8
FIELDS = 10
COLUMN_LAYERS = DEPTH_CLASSES * VERTICAL_LEVELS
GROUPS = (2, 3)
CHUNK = 4
OUT_CHUNK = 35
UNROLLED = 64
PARTS_TURN = 2
EDGE_KINDS = ((pl.ds(0, 2), HALO), (pl.ds(2, 4), HALO - 1), (pl.ds(6, 4), HALO - 2))
EDGE_ROWS = 2 * HALO + 4 * (HALO - 1) + 4 * (HALO - 2)

MESH = pl.DeviceIdType.MESH


def step_columns(temps, depth, surface, seawater):
    inverse = 1.0 / depth
    scaled = inverse * inverse
    base, salt = BASE_CONDUCT * scaled, SALT_CONDUCT * scaled
    half = 0.5 * salt
    guess = temps
    for turn in range(SWEEPS):
        if turn > 0:
            guess = back_substitute(ratio, done)
        turned = [1.0 / g for g in guess]
        coupling = [base + salt * turned[0]]
        for k in range(1, VERTICAL_LEVELS):
            coupling.append(base + half * (turned[k - 1] + turned[k]))
        coupling.append(base + salt * turned[-1])
        pivot = 1.0 + coupling[0]
        source = temps[0] + coupling[0] * surface
        ratio, done = [], []
        for k in range(VERTICAL_LEVELS):
            if k > 0:
                pivot = 1.0 + ratio[k - 1] * pivot
                source = temps[k] + ratio[k - 1] * source
            scale = 1.0 / (pivot + coupling[k + 1])
            if k < VERTICAL_LEVELS - 1:
                ratio.append(coupling[k + 1] * scale)
            else:
                source = source + coupling[k + 1] * FREEZE_POINT
            done.append(source * scale)
    bottom = done[-1]
    thick = (
        depth
        + GROWTH_RATE * (BASE_CONDUCT + SALT_CONDUCT / bottom) * (FREEZE_POINT - bottom) * inverse
        - seawater
    )
    return ratio, done, thick


def back_substitute(ratio, done):
    solved = list(done)
    for k in range(VERTICAL_LEVELS - 2, -1, -1):
        solved[k] = done[k] + ratio[k] * solved[k + 1]
    return solved


def shift(field, beside, amount):
    cols = field.shape[1] // 2
    lane = lax.broadcasted_iota(jnp.int32, (field.shape[0], cols), 1)
    crossing = lane == (0 if amount == 1 else cols - 1)
    turned = pltpu.roll(field[:, :cols], amount % cols, 1)
    return jnp.concatenate(
        [jnp.where(crossing, beside, turned), jnp.where(crossing, turned, beside)], axis=1
    )


def subcycle(moving, fixed, beside):
    u, v, s1, s2, s12 = moving
    strength, keep, push_scale, force_x, force_y = fixed
    rows, cols = u.shape[0], u.shape[1] // 2

    def lanes(f, amount):
        return pltpu.roll(f[:, cols:], amount % cols, 1)

    def dx(f, sides=None):
        sides = sides or (lanes(f, -1), lanes(f, 1))
        return shift(f, sides[0], -1) - shift(f, sides[1], 1)

    def dy(f):
        return pltpu.roll(f, rows - 1, 0) - pltpu.roll(f, 1, 0)

    ux, vy, uy, vx = dx(u, beside[0]), dy(v), dy(u), dx(v, beside[1])
    divergence = 0.5 * (ux + vy)
    tension = 0.5 * (ux - vy)
    shearing = 0.5 * (uy + vx)
    square = (
        divergence * divergence
        + (tension * tension + shearing * shearing) * (1.0 / ELLIPSE_SQUARE)
        + STRAIN_FLOOR
    )
    inverse = lax.rsqrt(square)
    deformation = square * inverse
    relax = 1.0 / (1.0 + STRESS_RELAX)
    viscous = (STRESS_RELAX * relax) * strength * inverse
    s1 = relax * s1 + viscous * (divergence - deformation)
    s2 = relax * s2 + viscous * tension * (1.0 / ELLIPSE_SQUARE)
    s12 = relax * s12 + viscous * shearing * (0.5 / ELLIPSE_SQUARE)
    push_x = dx(0.5 * (s1 + s2)) + dy(s12)
    push_y = dx(s12) + dy(0.5 * (s1 - s2))
    u = keep * u + push_scale * push_x + force_x
    v = keep * v + push_scale * push_y + force_y
    return u, v, s1, s2, s12


def as_column(row, rows):
    shape = (rows, rows)
    pick = lax.broadcasted_iota(jnp.int32, shape, 0) == lax.broadcasted_iota(jnp.int32, shape, 1)
    wide = jnp.broadcast_to(row.astype(jnp.float32), shape)
    return jnp.sum(jnp.where(pick, wide, 0.0), axis=1, keepdims=True)


def kernel(n_lat, n_lon, *refs):
    inputs, outputs, scratch = refs[:12], refs[12:17], refs[17:]
    temp_out, thick_out, vel_out, stress_out, zonal_out = outputs
    (held, strips, land_in, own, packed, edges, sides, parts) = scratch[:8]
    (in_sem, send_sem, recv_sem) = scratch[8:]
    rows, cols = land_in.shape
    devices = n_lat * n_lon
    lat, lon = lax.axis_index("lat"), lax.axis_index("lon")
    lats = [lax.rem(lat + d, n_lat) for d in range(n_lat)]
    lons = [lax.rem(lon + d, n_lon) for d in range(n_lon)]
    south, north, east, west = lats[1], lats[-1], lons[1], lons[-1]
    me = lon * n_lat + lat
    at_top, at_bottom = lat == 0, lat == n_lat - 1
    at_rim = at_top | at_bottom

    (temp_src, depth_src, area_src, surf_src, sea_src, vel_src, stress_src) = inputs[:7]
    (wind_src, current_src, land_src, ice_src, band_src) = inputs[7:]
    surf_in, sea_in = held.at[0], held.at[1]
    depth_at = range(2, 2 + DEPTH_CLASSES)
    area_at = range(2 + DEPTH_CLASSES, 2 + 2 * DEPTH_CLASSES)
    first_temp = 2 + 2 * DEPTH_CLASSES
    temp_at = range(first_temp, first_temp + COLUMN_LAYERS)
    temp_loads, blocks = [], []
    layer = 0
    for group, count in enumerate(GROUPS):
        end = layer + count * VERTICAL_LEVELS
        begin = first_temp + layer if group else 0
        blocks.append(held.at[pl.ds(begin, first_temp + end - begin)])
        temp_loads.append([])
        while layer < end:
            some = min(CHUNK, end - layer)
            temp_loads[group].append(
                (temp_src.at[pl.ds(layer, some)], held.at[pl.ds(first_temp + layer, some)], group)
            )
            layer += some
    start = first_temp + COLUMN_LAYERS
    last = len(GROUPS) - 1
    vel_in, stress_in = held.at[pl.ds(start, 2)], held.at[pl.ds(start + 2, 3)]
    wind_in, current_in = held.at[pl.ds(start + 5, 2)], held.at[pl.ds(start + 7, 2)]
    fast_loads = [
        (vel_src, vel_in, last + 3),
        (stress_src, stress_in, last + 3),
        (wind_src, wind_in, last + 3),
        (current_src, current_in, last + 3),
        (land_src, land_in, last + 2),
    ]
    loads = [
        (surf_src, surf_in, 0),
        (sea_src, sea_in, 0),
        (depth_src, held.at[pl.ds(2, DEPTH_CLASSES)], 0),
        *temp_loads[0],
        (area_src, held.at[pl.ds(2 + DEPTH_CLASSES, DEPTH_CLASSES)], 0),
        (band_src, strips.at[0], last + 1),
        (ice_src, strips.at[1], last + 1),
        *fast_loads,
        *[load for group in temp_loads[1:] for load in group],
    ]
    for source, target, group in loads:
        pltpu.make_async_copy(source, target, in_sem.at[group]).start()

    def arrive(ref, semaphore):
        pltpu.make_async_copy(ref, ref, semaphore).wait()

    def arrive_planes(inner, rim, semaphore):
        @pl.when(at_rim)
        def _():
            arrive(held.at[pl.ds(0, rim)], semaphore)

        @pl.when(jnp.logical_not(at_rim))
        def _():
            arrive(held.at[pl.ds(0, inner)], semaphore)

    pairs = [(a, g) for g in lons[1:] for a in lats] + [(a, lon) for a in lats[1:]]

    def everyone(visit):
        def step(d, carry):
            other = lax.rem(me + 1 + d, devices)
            visit((lax.rem(other, n_lat), other // n_lat))
            return carry

        lax.fori_loop(0, devices - 1, step, 0)

    barrier = pltpu.get_barrier_semaphore()

    def greet(device):
        pl.semaphore_signal(barrier, inc=1, device_id=device, device_id_type=MESH)

    if devices <= UNROLLED:
        for pair in pairs[1 - n_lat :] + pairs[: 1 - n_lat]:
            greet(pair)
    else:
        everyone(greet)

    kept = []

    def thermo(c):
        temps = [held[temp_at[c * VERTICAL_LEVELS + k]] for k in range(VERTICAL_LEVELS)]
        depth = held[depth_at[c]]
        ratio, done, thick = step_columns(temps, depth, surf_in[...], sea_in[...])
        kept.append((ratio, done, thick))

    def finish_temps(c):
        for k, solved in enumerate(back_substitute(*kept[c][:2])):
            temp = held[temp_at[c * VERTICAL_LEVELS + k]]
            temp_out[c * VERTICAL_LEVELS + k] = jnp.where(icy, solved, temp)

    def send_part(device):
        pltpu.make_async_remote_copy(
            src_ref=parts.at[pl.ds(me, 1)],
            dst_ref=parts.at[pl.ds(me, 1)],
            send_sem=send_sem.at[0],
            recv_sem=recv_sem.at[0],
            device_id=device,
            device_id_type=MESH,
        ).start()

    def send_halo(source, target, device, arrival):
        pltpu.make_async_remote_copy(
            src_ref=source,
            dst_ref=target,
            send_sem=send_sem.at[1],
            recv_sem=recv_sem.at[arrival],
            device_id=device,
            device_id_type=MESH,
        ).start()

    arrive(blocks[0], in_sem.at[0])
    for c in range(0, 2):
        thermo(c)
    arrive(blocks[1], in_sem.at[1])
    arrive(held.at[pl.ds(start, 9)], in_sem.at[last + 3])
    arrive(land_in, in_sem.at[last + 2])
    arrive(strips, in_sem.at[last + 1])
    icy = as_column(strips[1], rows) == 1.0
    width = parts.shape[-1]
    band = as_column(strips[0], rows).astype(jnp.int32)
    slot = lax.broadcasted_iota(jnp.int32, (rows, width), 1)
    member = band == slot
    counted = jnp.where(band + width // 2 == slot, float(cols), 0.0)

    for c in range(2, 5):
        thermo(c)
    volume = held[area_at[0]] * held[depth_at[0]]
    coverage = held[area_at[0]]
    for c in range(1, DEPTH_CLASSES):
        volume = volume + held[area_at[c]] * held[depth_at[c]]
        coverage = coverage + held[area_at[c]]
    strength = volume * jnp.exp(-STRENGTH_DECAY * (1.0 - coverage))
    drag = 1.0 / (1.0 + MOMENTUM_STEP * WATER_DRAG)
    keep = land_in[...].astype(jnp.float32) * drag
    forced = MOMENTUM_STEP * keep
    push_scale = 0.5 * forced / (1.0 + volume)
    fields = [vel_in[0], vel_in[1], stress_in[0], stress_in[1], stress_in[2], strength, keep]
    fields += [push_scale]
    fields += [forced * (wind_in[i] + WATER_DRAG * current_in[i]) for i in range(2)]
    lane = lax.broadcasted_iota(jnp.int32, (rows, cols), 1)
    pack = jnp.zeros((rows, cols), jnp.float32)
    for f in range(FIELDS):
        first = 2 * HALO * f
        turned = pltpu.roll(fields[f], (first + HALO) % cols, 1)
        pack = jnp.where((lane >= first) & (lane < first + 2 * HALO), turned, pack)
    packed[...] = pack
    for f in range(FIELDS):
        own[f] = fields[f]

    after = jnp.zeros((rows, cols), jnp.float32)
    for c in range(DEPTH_CLASSES):
        thick = jnp.where(icy, kept[c][2], held[depth_at[c]])
        thick_out[c] = thick
        after = after + held[area_at[c]] * thick
    total = jnp.sum(after, axis=1, keepdims=True)
    parts[pl.ds(me, 1)] = jnp.sum(jnp.where(member, total, counted), axis=0, keepdims=True)
    pl.semaphore_wait(barrier, devices - 1)

    if devices <= UNROLLED:
        for pair in pairs[0:4]:
            send_part(pair)

    tail, head = pl.ds(rows - EDGE, EDGE), pl.ds(0, EDGE)
    above, middle, below = pl.ds(0, EDGE), pl.ds(EDGE, rows), pl.ds(EDGE + rows, EDGE)
    send_halo(packed, sides.at[0, middle], (lat, east), 1)
    send_halo(packed, sides.at[1, middle], (lat, west), 1)

    @pl.when(jnp.logical_not(at_bottom))
    def _():
        send_halo(packed.at[tail], sides.at[0, above], (south, east), 1)
        send_halo(packed.at[tail], sides.at[1, above], (south, west), 1)
        for kind, reach in EDGE_KINDS:
            send_halo(
                own.at[kind, pl.ds(rows - reach, reach)],
                edges.at[0, kind, pl.ds(EDGE - reach, reach)],
                (south, lon),
                2,
            )

    @pl.when(jnp.logical_not(at_top))
    def _():
        send_halo(packed.at[head], sides.at[0, below], (north, east), 1)
        send_halo(packed.at[head], sides.at[1, below], (north, west), 1)
        for kind, reach in EDGE_KINDS:
            send_halo(
                own.at[kind, pl.ds(0, reach)],
                edges.at[1, kind, pl.ds(0, reach)],
                (north, lon),
                2,
            )

    if devices <= UNROLLED:
        for pair in pairs[4:]:
            send_part(pair)
    else:
        everyone(send_part)

    for c in range(DEPTH_CLASSES):
        finish_temps(c)

    def finish_zonal():
        whole = jnp.sum(parts[...], axis=0, keepdims=True)
        whole = pltpu.roll(whole, lax.rem(width - lat * BANDS_DEV, width), 1)
        cells = pltpu.roll(whole, width // 2, 1)
        mean = whole / jnp.maximum(cells, 1.0)
        zonal_out[...] = mean[:, :BANDS_DEV]

    brim = EDGE_ROWS // rows
    arrive_planes(2 * brim, brim, recv_sem.at[2])
    arrive_planes(4, 3, recv_sem.at[1])
    tall = rows + 2 * EDGE
    low = jnp.where(at_top, EDGE, 0)
    high = jnp.where(at_bottom, EDGE + rows, tall)
    row_id = lax.broadcasted_iota(jnp.int32, (tall, cols), 0)
    inside = (row_id >= low) & (row_id < high)
    place = lax.broadcasted_iota(jnp.int32, (tall, cols), 1)
    merged = jnp.where(lax.rem(place, 2 * HALO) < HALO, sides[0], sides[1])
    merged = jnp.where(inside, merged, 0.0)

    def beside(f, amount):
        return pltpu.roll(merged, (2 * cols - 2 * HALO * f - HALO + amount) % cols, 1)

    state = []
    for f in range(FIELDS):
        centre = jnp.concatenate([edges[0, f], own[f], edges[1, f]], axis=0)
        centre = jnp.where(inside, centre, 0.0)
        state.append(jnp.concatenate([centre, beside(f, 0)], axis=1))
    moving, fixed = state[:5], state[5:]
    first_beside = [(beside(f, -1), beside(f, 1)) for f in range(2)]
    others = parts.at[pl.ds(0, devices - 1)]
    for turn in range(SUBCYCLES):
        if turn == PARTS_TURN:
            arrive(others, recv_sem.at[0])
            finish_zonal()
        moving = subcycle(moving, fixed, first_beside if turn == 0 else (None, None))
    for i in range(2):
        vel_out[i] = moving[i][EDGE : EDGE + rows, :cols]
    for i in range(3):
        stress_out[i] = moving[2 + i][EDGE : EDGE + rows, :cols]

    if PARTS_TURN == SUBCYCLES:
        arrive(others, recv_sem.at[0])
        finish_zonal()
    arrive_planes(2 + 2 * (brim + 1), 2 + brim + 1, send_sem.at[1])
    arrive(others, send_sem.at[0])


def put_out(temp, thick, vel, stress, zonal, *refs):
    outs, sem = refs[:5], refs[5]
    planes = [ref.shape[0] for ref in (thick, vel, stress)]
    copies = [(zonal, outs[4], 2), (vel, outs[2], 1), (stress, outs[3], 1), (thick, outs[1], 1)]
    for first in range(0, COLUMN_LAYERS, OUT_CHUNK):
        some = pl.ds(first, min(OUT_CHUNK, COLUMN_LAYERS - first))
        copies.append((temp.at[some], outs[0].at[some], 0))
    for source, target, group in copies:
        pltpu.make_async_copy(source, target, sem.at[group]).start()
    pltpu.make_async_copy(temp, outs[0], sem.at[0]).wait()
    small = pl.ds(0, sum(planes))
    pltpu.make_async_copy(temp.at[small], outs[0].at[small], sem.at[1]).wait()
    pltpu.make_async_copy(zonal, outs[4], sem.at[2]).wait()


def local(n_lat, n_lon, *args):
    args = list(args)
    args[:3] = [jnp.transpose(a, (1, 0, 2)) for a in args[:3]]
    args[11] = args[11].reshape(1, -1)
    rows, cols = args[3].shape
    width = -(-2 * BANDS_DEV * n_lat // cols) * cols
    tall = rows + 2 * EDGE
    f32 = jnp.float32
    vmem = pl.BlockSpec(memory_space=pltpu.VMEM)
    shapes = [args[i].shape for i in (0, 1, 5, 6)] + [(1, BANDS_DEV)]
    dma = pltpu.SemaphoreType.DMA
    results = pl.pallas_call(
        functools.partial(kernel, n_lat, n_lon),
        out_shape=[pltpu.VMEM(shape, f32) for shape in shapes],
        in_specs=[pl.BlockSpec(memory_space=pl.ANY)] * 12,
        out_specs=[vmem] * 5,
        scratch_shapes=[
            pltpu.VMEM((2 * DEPTH_CLASSES + 2 + COLUMN_LAYERS + 9, rows, cols), f32),
            pltpu.VMEM((2, 1, rows), jnp.int32),
            pltpu.VMEM((rows, cols), jnp.int32),
            pltpu.VMEM((FIELDS, rows, cols), f32),
            pltpu.VMEM((rows, cols), f32),
            pltpu.VMEM((2, FIELDS, EDGE, cols), f32),
            pltpu.VMEM((2, tall, cols), f32),
            pltpu.VMEM((n_lat * n_lon, width), f32),
            dma((len(GROUPS) + 3,)),
            dma((2,)),
            dma((3,)),
        ],
        compiler_params=pltpu.CompilerParams(collective_id=0, has_side_effects=True),
        name="ice_step",
    )(*args)
    temp, thick, vel, stress, zonal = pl.pallas_call(
        put_out,
        out_shape=[jax.ShapeDtypeStruct(shape, f32) for shape in shapes],
        in_specs=[vmem] * 5,
        out_specs=[pl.BlockSpec(memory_space=pl.ANY)] * 5,
        scratch_shapes=[dma((3,))],
        name="put_out",
    )(*[pltpu.with_memory_space_constraint(r, pltpu.VMEM) for r in results])
    temp, thick = [jnp.transpose(a, (1, 0, 2)) for a in (temp, thick)]
    return (temp, thick, vel, stress, zonal.reshape(BANDS_DEV))


def solution(mesh):
    shape = dict(mesh.shape)
    return jax.shard_map(
        functools.partial(local, shape["lat"], shape["lon"]),
        mesh=mesh,
        in_specs=(
            P("lat", None, "lon"),
            P("lat", None, "lon"),
            P("lat", None, "lon"),
            P("lat", "lon"),
            P("lat", "lon"),
            P(None, "lat", "lon"),
            P(None, "lat", "lon"),
            P(None, "lat", "lon"),
            P(None, "lat", "lon"),
            P("lat", "lon"),
            P("lon", "lat"),
            P("lat"),
        ),
        out_specs=(
            P("lat", None, "lon"),
            P("lat", None, "lon"),
            P(None, "lat", "lon"),
            P(None, "lat", "lon"),
            P("lat"),
        ),
        check_vma=False,
    )
```

```python
import functools

import jax
import jax.numpy as jnp
from jax import lax
from jax.experimental import pallas as pl
from jax.experimental.pallas import tpu as pltpu
from jax.sharding import PartitionSpec as P

DEPTH_CLASSES = 5
VERTICAL_LEVELS = 7
SUBCYCLES = 3
SWEEPS = 2
BANDS_DEV = 4

FREEZE_POINT = -1.8
BASE_CONDUCT = 2.03
SALT_CONDUCT = 0.416
GROWTH_RATE = 0.02
STRENGTH_DECAY = 5.0
ELLIPSE_SQUARE = 4.0
STRAIN_FLOOR = 0.0025
STRESS_RELAX = 0.5
MOMENTUM_STEP = 0.5
WATER_DRAG = 1.0

HALO = 2 * SUBCYCLES
EDGE = 8
FIELDS = 10
COLUMN_LAYERS = DEPTH_CLASSES * VERTICAL_LEVELS
GROUPS = (2, 3)
FAST = 2 * DEPTH_CLASSES + 9
CHUNK = 4
OUT_CHUNK = 4
UNROLLED = 64
PARTS_TURN = 3
EDGE_KINDS = ((pl.ds(0, 2), HALO), (pl.ds(2, 4), HALO - 1), (pl.ds(6, 4), HALO - 2))
EDGE_ROWS = 2 * HALO + 4 * (HALO - 1) + 4 * (HALO - 2)

MESH = pl.DeviceIdType.MESH


def step_columns(temps, depth, surface, seawater):
    inverse = 1.0 / depth
    scaled = inverse * inverse
    base, salt = BASE_CONDUCT * scaled, SALT_CONDUCT * scaled
    half = 0.5 * salt
    guess = temps
    for turn in range(SWEEPS):
        if turn > 0:
            guess = back_substitute(ratio, done)
        turned = [1.0 / g for g in guess]
        coupling = [base + salt * turned[0]]
        for k in range(1, VERTICAL_LEVELS):
            coupling.append(base + half * (turned[k - 1] + turned[k]))
        coupling.append(base + salt * turned[-1])
        pivot = 1.0 + coupling[0]
        source = temps[0] + coupling[0] * surface
        ratio, done = [], []
        for k in range(VERTICAL_LEVELS):
            if k > 0:
                pivot = 1.0 + ratio[k - 1] * pivot
                source = temps[k] + ratio[k - 1] * source
            scale = 1.0 / (pivot + coupling[k + 1])
            if k < VERTICAL_LEVELS - 1:
                ratio.append(coupling[k + 1] * scale)
            else:
                source = source + coupling[k + 1] * FREEZE_POINT
            done.append(source * scale)
    bottom = done[-1]
    thick = (
        depth
        + GROWTH_RATE * (BASE_CONDUCT + SALT_CONDUCT / bottom) * (FREEZE_POINT - bottom) * inverse
        - seawater
    )
    return ratio, done, thick


def back_substitute(ratio, done):
    solved = list(done)
    for k in range(VERTICAL_LEVELS - 2, -1, -1):
        solved[k] = done[k] + ratio[k] * solved[k + 1]
    return solved


def shift(field, beside, amount):
    cols = field.shape[1] // 2
    lane = lax.broadcasted_iota(jnp.int32, (field.shape[0], cols), 1)
    crossing = lane == (0 if amount == 1 else cols - 1)
    turned = pltpu.roll(field[:, :cols], amount % cols, 1)
    return jnp.concatenate(
        [jnp.where(crossing, beside, turned), jnp.where(crossing, turned, beside)], axis=1
    )


def subcycle(moving, fixed, beside):
    u, v, s1, s2, s12 = moving
    strength, keep, push_scale, force_x, force_y = fixed
    rows, cols = u.shape[0], u.shape[1] // 2

    def lanes(f, amount):
        return pltpu.roll(f[:, cols:], amount % cols, 1)

    def dx(f, sides=None):
        sides = sides or (lanes(f, -1), lanes(f, 1))
        return shift(f, sides[0], -1) - shift(f, sides[1], 1)

    def dy(f):
        return pltpu.roll(f, rows - 1, 0) - pltpu.roll(f, 1, 0)

    ux, vy, uy, vx = dx(u, beside[0]), dy(v), dy(u), dx(v, beside[1])
    divergence = 0.5 * (ux + vy)
    tension = 0.5 * (ux - vy)
    shearing = 0.5 * (uy + vx)
    square = (
        divergence * divergence
        + (tension * tension + shearing * shearing) * (1.0 / ELLIPSE_SQUARE)
        + STRAIN_FLOOR
    )
    inverse = lax.rsqrt(square)
    deformation = square * inverse
    relax = 1.0 / (1.0 + STRESS_RELAX)
    viscous = (STRESS_RELAX * relax) * strength * inverse
    s1 = relax * s1 + viscous * (divergence - deformation)
    s2 = relax * s2 + viscous * tension * (1.0 / ELLIPSE_SQUARE)
    s12 = relax * s12 + viscous * shearing * (0.5 / ELLIPSE_SQUARE)
    push_x = dx(0.5 * (s1 + s2)) + dy(s12)
    push_y = dx(s12) + dy(0.5 * (s1 - s2))
    u = keep * u + push_scale * push_x + force_x
    v = keep * v + push_scale * push_y + force_y
    return u, v, s1, s2, s12


def as_column(row, rows):
    shape = (rows, rows)
    pick = lax.broadcasted_iota(jnp.int32, shape, 0) == lax.broadcasted_iota(jnp.int32, shape, 1)
    wide = jnp.broadcast_to(row.astype(jnp.float32), shape)
    return jnp.sum(jnp.where(pick, wide, 0.0), axis=1, keepdims=True)


def kernel(n_lat, n_lon, *refs):
    inputs, outputs, scratch = refs[:12], refs[12:17], refs[17:]
    temp_out, thick_out, vel_out, stress_out, zonal_out = outputs
    (held, strips, land_in, own, packed, edges, sides, parts, outbox) = scratch[:9]
    (in_sem, send_sem, recv_sem) = scratch[9:]
    rows, cols = land_in.shape
    devices = n_lat * n_lon
    lat, lon = lax.axis_index("lat"), lax.axis_index("lon")
    lats = [lax.rem(lat + d, n_lat) for d in range(n_lat)]
    lons = [lax.rem(lon + d, n_lon) for d in range(n_lon)]
    south, north, east, west = lats[1], lats[-1], lons[1], lons[-1]
    me = lon * n_lat + lat
    at_top, at_bottom = lat == 0, lat == n_lat - 1
    at_rim = at_top | at_bottom

    (temp_src, depth_src, area_src, surf_src, sea_src, vel_src, stress_src) = inputs[:7]
    (wind_src, current_src, land_src, ice_src, band_src) = inputs[7:]
    surf_in, sea_in = held.at[FAST], held.at[FAST + 1]
    depth_at = range(DEPTH_CLASSES)
    area_at = range(DEPTH_CLASSES, 2 * DEPTH_CLASSES)
    first_temp = FAST + 2
    temp_at = range(first_temp, first_temp + COLUMN_LAYERS)
    temp_loads, blocks = [], []
    layer = 0
    for group, count in enumerate(GROUPS):
        end = layer + count * VERTICAL_LEVELS
        begin = first_temp + layer if group else FAST
        blocks.append(held.at[pl.ds(begin, first_temp + end - begin)])
        temp_loads.append([])
        while layer < end:
            some = min(CHUNK, end - layer)
            temp_loads[group].append(
                (temp_src.at[pl.ds(layer, some)], held.at[pl.ds(first_temp + layer, some)], group)
            )
            layer += some
    start = 2 * DEPTH_CLASSES
    last = len(GROUPS) - 1
    vel_in, stress_in = held.at[pl.ds(start, 2)], held.at[pl.ds(start + 2, 3)]
    wind_in, current_in = held.at[pl.ds(start + 5, 2)], held.at[pl.ds(start + 7, 2)]
    fast_loads = [
        (vel_src, vel_in, last + 3),
        (stress_src, stress_in, last + 3),
        (wind_src, wind_in, last + 3),
        (current_src, current_in, last + 3),
        (land_src, land_in, last + 2),
    ]
    loads = [
        *fast_loads,
        (depth_src, held.at[pl.ds(0, DEPTH_CLASSES)], last + 3),
        (area_src, held.at[pl.ds(DEPTH_CLASSES, DEPTH_CLASSES)], last + 3),
        (surf_src, surf_in, 0),
        (sea_src, sea_in, 0),
        *temp_loads[0],
        (band_src, strips.at[0], last + 1),
        (ice_src, strips.at[1], last + 1),
        *[load for group in temp_loads[1:] for load in group],
    ]
    for source, target, group in loads:
        pltpu.make_async_copy(source, target, in_sem.at[group]).start()

    def arrive(ref, semaphore):
        pltpu.make_async_copy(ref, ref, semaphore).wait()

    def arrive_planes(inner, rim, semaphore):
        @pl.when(at_rim)
        def _():
            arrive(held.at[pl.ds(0, rim)], semaphore)

        @pl.when(jnp.logical_not(at_rim))
        def _():
            arrive(held.at[pl.ds(0, inner)], semaphore)

    pairs = [(a, g) for g in lons[1:] for a in lats[n_lat // 2 :] + lats[: n_lat // 2]] + [(a, lon) for a in lats[1:]]

    def everyone(visit):
        def step(d, carry):
            other = lax.rem(me + 1 + d, devices)
            visit((lax.rem(other, n_lat), other // n_lat))
            return carry

        lax.fori_loop(0, devices - 1, step, 0)

    barrier = pltpu.get_barrier_semaphore()

    def greet(device):
        pl.semaphore_signal(barrier, inc=1, device_id=device, device_id_type=MESH)

    if devices <= UNROLLED:
        for pair in pairs[1 - n_lat :] + pairs[: 1 - n_lat]:
            greet(pair)
    else:
        everyone(greet)

    kept = []

    def thermo(c):
        temps = [held[temp_at[c * VERTICAL_LEVELS + k]] for k in range(VERTICAL_LEVELS)]
        depth = held[depth_at[c]]
        ratio, done, thick = step_columns(temps, depth, surf_in[...], sea_in[...])
        kept.append((ratio, done, thick))

    def finish_temps(c):
        for k, solved in enumerate(back_substitute(*kept[c][:2])):
            temp = held[temp_at[c * VERTICAL_LEVELS + k]]
            temp_out[c * VERTICAL_LEVELS + k] = jnp.where(icy, solved, temp)

    def send_part(device):
        pltpu.make_async_remote_copy(
            src_ref=outbox.at[pl.ds(2 * device[0], 2)],
            dst_ref=parts.at[pl.ds(2 * me, 2)],
            send_sem=send_sem.at[0],
            recv_sem=recv_sem.at[0],
            device_id=device,
            device_id_type=MESH,
        ).start()

    def send_halo(source, target, device, arrival):
        pltpu.make_async_remote_copy(
            src_ref=source,
            dst_ref=target,
            send_sem=send_sem.at[1],
            recv_sem=recv_sem.at[arrival],
            device_id=device,
            device_id_type=MESH,
        ).start()

    arrive(held.at[pl.ds(0, FAST)], in_sem.at[last + 3])
    arrive(land_in, in_sem.at[last + 2])
    arrive(blocks[0], in_sem.at[0])
    volume = held[area_at[0]] * held[depth_at[0]]
    coverage = held[area_at[0]]
    for c in range(1, DEPTH_CLASSES):
        volume = volume + held[area_at[c]] * held[depth_at[c]]
        coverage = coverage + held[area_at[c]]
    strength = volume * jnp.exp(-STRENGTH_DECAY * (1.0 - coverage))
    drag = 1.0 / (1.0 + MOMENTUM_STEP * WATER_DRAG)
    keep = land_in[...].astype(jnp.float32) * drag
    forced = MOMENTUM_STEP * keep
    push_scale = 0.5 * forced / (1.0 + volume)
    fields = [vel_in[0], vel_in[1], stress_in[0], stress_in[1], stress_in[2], strength, keep]
    fields += [push_scale]
    fields += [forced * (wind_in[i] + WATER_DRAG * current_in[i]) for i in range(2)]
    lane = lax.broadcasted_iota(jnp.int32, (rows, cols), 1)
    pack = jnp.zeros((rows, cols), jnp.float32)
    for f in range(FIELDS):
        first = 2 * HALO * f
        turned = pltpu.roll(fields[f], (first + HALO) % cols, 1)
        pack = jnp.where((lane >= first) & (lane < first + 2 * HALO), turned, pack)
    packed[...] = pack
    for f in range(FIELDS):
        own[f] = fields[f]

    for c in range(0, 2):
        thermo(c)
    pl.semaphore_wait(barrier, devices - 1)

    tail, head = pl.ds(rows - EDGE, EDGE), pl.ds(0, EDGE)
    above, middle, below = pl.ds(0, EDGE), pl.ds(EDGE, rows), pl.ds(EDGE + rows, EDGE)
    send_halo(packed, sides.at[0, middle], (lat, east), 1)
    send_halo(packed, sides.at[1, middle], (lat, west), 1)

    @pl.when(jnp.logical_not(at_bottom))
    def _():
        send_halo(packed.at[tail], sides.at[0, above], (south, east), 1)
        send_halo(packed.at[tail], sides.at[1, above], (south, west), 1)
        for kind, reach in EDGE_KINDS:
            send_halo(
                own.at[kind, pl.ds(rows - reach, reach)],
                edges.at[0, kind, pl.ds(EDGE - reach, reach)],
                (south, lon),
                2,
            )

    @pl.when(jnp.logical_not(at_top))
    def _():
        send_halo(packed.at[head], sides.at[0, below], (north, east), 1)
        send_halo(packed.at[head], sides.at[1, below], (north, west), 1)
        for kind, reach in EDGE_KINDS:
            send_halo(
                own.at[kind, pl.ds(0, reach)],
                edges.at[1, kind, pl.ds(0, reach)],
                (north, lon),
                2,
            )

    arrive(blocks[1], in_sem.at[1])
    arrive(strips, in_sem.at[last + 1])
    icy = as_column(strips[1], rows) == 1.0
    band = as_column(strips[0], rows).astype(jnp.int32)
    slot = lax.broadcasted_iota(jnp.int32, (rows, cols), 1)
    slot = jnp.where(slot < BANDS_DEV, slot, -BANDS_DEV * n_lat)
    members = [band - BANDS_DEV * a == slot for a in range(n_lat)]
    for a in range(n_lat):
        counted = jnp.where(members[a], float(cols), 0.0)
        outbox[pl.ds(2 * a + 1, 1)] = jnp.sum(counted, axis=0, keepdims=True)

    for c in range(2, 5):
        thermo(c)
    after = jnp.zeros((rows, cols), jnp.float32)
    for c in range(DEPTH_CLASSES):
        thick = jnp.where(icy, kept[c][2], held[depth_at[c]])
        thick_out[c] = thick
        after = after + held[area_at[c]] * thick
    total = jnp.sum(after, axis=1, keepdims=True)
    for a in range(n_lat):
        outbox[pl.ds(2 * a, 1)] = jnp.sum(jnp.where(members[a], total, 0.0), axis=0, keepdims=True)
    if devices <= UNROLLED:
        for pair in pairs[0:]:
            send_part(pair)
    else:
        everyone(send_part)

    for c in range(DEPTH_CLASSES):
        finish_temps(c)

    parts[pl.ds(2 * me, 2)] = outbox[pl.ds(2 * lat, 2)]

    def finish_zonal():
        whole = jnp.sum(parts[...].reshape(-1, 8, cols), axis=0)
        whole = whole + pltpu.roll(whole, 4, 0)
        whole = whole + pltpu.roll(whole, 2, 0)
        mean = whole[:1] / jnp.maximum(whole[1:2], 1.0)
        zonal_out[...] = mean[:, :BANDS_DEV]

    brim = EDGE_ROWS // rows
    arrive_planes(2 * brim, brim, recv_sem.at[2])
    arrive_planes(4, 3, recv_sem.at[1])
    tall = rows + 2 * EDGE
    low = jnp.where(at_top, EDGE, 0)
    high = jnp.where(at_bottom, EDGE + rows, tall)
    row_id = lax.broadcasted_iota(jnp.int32, (tall, cols), 0)
    inside = (row_id >= low) & (row_id < high)
    place = lax.broadcasted_iota(jnp.int32, (tall, cols), 1)
    merged = jnp.where(lax.rem(place, 2 * HALO) < HALO, sides[0], sides[1])
    merged = jnp.where(inside, merged, 0.0)

    def beside(f, amount):
        return pltpu.roll(merged, (2 * cols - 2 * HALO * f - HALO + amount) % cols, 1)

    state = []
    for f in range(FIELDS):
        centre = jnp.concatenate([edges[0, f], own[f], edges[1, f]], axis=0)
        centre = jnp.where(inside, centre, 0.0)
        state.append(jnp.concatenate([centre, beside(f, 0)], axis=1))
    moving, fixed = state[:5], state[5:]
    first_beside = [(beside(f, -1), beside(f, 1)) for f in range(2)]
    others = parts.at[pl.ds(0, 2 * (devices - 1))]
    for turn in range(SUBCYCLES):
        if turn == PARTS_TURN:
            arrive(others, recv_sem.at[0])
            finish_zonal()
        moving = subcycle(moving, fixed, first_beside if turn == 0 else (None, None))
    for i in range(2):
        vel_out[i] = moving[i][EDGE : EDGE + rows, :cols]
    for i in range(3):
        stress_out[i] = moving[2 + i][EDGE : EDGE + rows, :cols]

    arrive_planes(2 + 2 * (brim + 1), 2 + brim + 1, send_sem.at[1])
    arrive(others, send_sem.at[0])
    if PARTS_TURN == SUBCYCLES:
        arrive(others, recv_sem.at[0])
        finish_zonal()


def put_out(temp, thick, vel, stress, zonal, *refs):
    outs, sem = refs[:5], refs[5]
    planes = [ref.shape[0] for ref in (thick, vel, stress)]
    copies = [(zonal, outs[4], 2), (vel, outs[2], 1), (stress, outs[3], 1), (thick, outs[1], 1)]
    for first in range(0, COLUMN_LAYERS, OUT_CHUNK):
        some = pl.ds(first, min(OUT_CHUNK, COLUMN_LAYERS - first))
        copies.append((temp.at[some], outs[0].at[some], 0))
    for source, target, group in copies:
        pltpu.make_async_copy(source, target, sem.at[group]).start()
    pltpu.make_async_copy(temp, outs[0], sem.at[0]).wait()
    small = pl.ds(0, sum(planes))
    pltpu.make_async_copy(temp.at[small], outs[0].at[small], sem.at[1]).wait()
    pltpu.make_async_copy(zonal, outs[4], sem.at[2]).wait()


def local(n_lat, n_lon, *args):
    args = list(args)
    args[:3] = [jnp.transpose(a, (1, 0, 2)) for a in args[:3]]
    args[11] = args[11].reshape(1, -1)
    rows, cols = args[3].shape
    tall = rows + 2 * EDGE
    f32 = jnp.float32
    vmem = pl.BlockSpec(memory_space=pltpu.VMEM)
    shapes = [args[i].shape for i in (0, 1, 5, 6)] + [(1, BANDS_DEV)]
    dma = pltpu.SemaphoreType.DMA
    results = pl.pallas_call(
        functools.partial(kernel, n_lat, n_lon),
        out_shape=[pltpu.VMEM(shape, f32) for shape in shapes],
        in_specs=[pl.BlockSpec(memory_space=pl.ANY)] * 12,
        out_specs=[vmem] * 5,
        scratch_shapes=[
            pltpu.VMEM((2 * DEPTH_CLASSES + 2 + COLUMN_LAYERS + 9, rows, cols), f32),
            pltpu.VMEM((2, 1, rows), jnp.int32),
            pltpu.VMEM((rows, cols), jnp.int32),
            pltpu.VMEM((FIELDS, rows, cols), f32),
            pltpu.VMEM((rows, cols), f32),
            pltpu.VMEM((2, FIELDS, EDGE, cols), f32),
            pltpu.VMEM((2, tall, cols), f32),
            pltpu.VMEM((2 * n_lat * n_lon, cols), f32),
            pltpu.VMEM((2 * n_lat, cols), f32),
            dma((len(GROUPS) + 3,)),
            dma((2,)),
            dma((3,)),
        ],
        compiler_params=pltpu.CompilerParams(collective_id=0, has_side_effects=True),
        name="ice_step",
    )(*args)
    temp, thick, vel, stress, zonal = pl.pallas_call(
        put_out,
        out_shape=[jax.ShapeDtypeStruct(shape, f32) for shape in shapes],
        in_specs=[vmem] * 5,
        out_specs=[pl.BlockSpec(memory_space=pl.ANY)] * 5,
        scratch_shapes=[dma((3,))],
        name="put_out",
    )(*[pltpu.with_memory_space_constraint(r, pltpu.VMEM) for r in results])
    temp, thick = [jnp.transpose(a, (1, 0, 2)) for a in (temp, thick)]
    return (temp, thick, vel, stress, zonal.reshape(BANDS_DEV))


def solution(mesh):
    shape = dict(mesh.shape)
    return jax.shard_map(
        functools.partial(local, shape["lat"], shape["lon"]),
        mesh=mesh,
        in_specs=(
            P("lat", None, "lon"),
            P("lat", None, "lon"),
            P("lat", None, "lon"),
            P("lat", "lon"),
            P("lat", "lon"),
            P(None, "lat", "lon"),
            P(None, "lat", "lon"),
            P(None, "lat", "lon"),
            P(None, "lat", "lon"),
            P("lat", "lon"),
            P("lon", "lat"),
            P("lat"),
        ),
        out_specs=(
            P("lat", None, "lon"),
            P("lat", None, "lon"),
            P(None, "lat", "lon"),
            P(None, "lat", "lon"),
            P("lat"),
        ),
        check_vma=False,
    )
```

```python
import functools

import jax
import jax.numpy as jnp
from jax import lax
from jax.experimental import pallas as pl
from jax.experimental.pallas import tpu as pltpu
from jax.sharding import PartitionSpec as P

DEPTH_CLASSES = 5
VERTICAL_LEVELS = 7
SUBCYCLES = 3
SWEEPS = 2
BANDS_DEV = 4

FREEZE_POINT = -1.8
BASE_CONDUCT = 2.03
SALT_CONDUCT = 0.416
GROWTH_RATE = 0.02
STRENGTH_DECAY = 5.0
ELLIPSE_SQUARE = 4.0
STRAIN_FLOOR = 0.0025
STRESS_RELAX = 0.5
MOMENTUM_STEP = 0.5
WATER_DRAG = 1.0

HALO = 2 * SUBCYCLES
EDGE = 8
FIELDS = 10
COLUMN_LAYERS = DEPTH_CLASSES * VERTICAL_LEVELS
GROUPS = (2, 3)
FAST = 2 * DEPTH_CLASSES + 9
CHUNK = 4
OUT_CHUNK = 4
UNROLLED = 64
PARTS_TURN = 3
EDGE_KINDS = ((pl.ds(0, 6), HALO), (pl.ds(6, 4), HALO + 1))
EDGE_ROWS = 6 * HALO + 4 * (HALO + 1)

MESH = pl.DeviceIdType.MESH


def eliminate(temps, outside, coupling):
    pivot = 1.0 + coupling[0]
    source = temps[0] + coupling[0] * outside
    ratio, done = [], []
    for k in range(1, len(temps)):
        scale = 1.0 / (pivot + coupling[k])
        ratio.append(coupling[k] * scale)
        done.append(source * scale)
        pivot = 1.0 + ratio[-1] * pivot
        source = temps[k] + ratio[-1] * source
    return ratio, done, pivot, source


def meet(temps, surface, coupling):
    mid = VERTICAL_LEVELS // 2
    upper, above, pivot, source = eliminate(temps[: mid + 1], surface, coupling)
    lower, below, pivot_low, source_low = eliminate(temps[:mid:-1], FREEZE_POINT, coupling[::-1])
    scale = 1.0 / (pivot_low + coupling[mid + 1])
    lower.append(coupling[mid + 1] * scale)
    below.append(source_low * scale)
    middle = (source + lower[-1] * source_low) / (pivot + lower[-1] * pivot_low)
    solved = [middle]
    for k in range(mid - 1, -1, -1):
        solved.insert(0, above[k] + upper[k] * solved[0])
    for k in range(len(below) - 1, -1, -1):
        solved.append(below[k] + lower[k] * solved[-1])
    return solved


def step_columns(temps, depth, surface, seawater):
    inverse = 1.0 / depth
    scaled = inverse * inverse
    base, salt = BASE_CONDUCT * scaled, SALT_CONDUCT * scaled
    half = 0.5 * salt
    guess = temps
    for turn in range(SWEEPS):
        turned = [1.0 / g for g in guess]
        coupling = [base + salt * turned[0]]
        for k in range(1, VERTICAL_LEVELS):
            coupling.append(base + half * (turned[k - 1] + turned[k]))
        coupling.append(base + salt * turned[-1])
        if turn < SWEEPS - 1:
            guess = meet(temps, surface, coupling)
    ratio, done, pivot, source = eliminate(temps, surface, coupling)
    bottom = (source + coupling[-1] * FREEZE_POINT) / (pivot + coupling[-1])
    done.append(bottom)
    thick = (
        depth
        + GROWTH_RATE * (BASE_CONDUCT + SALT_CONDUCT / bottom) * (FREEZE_POINT - bottom) * inverse
        - seawater
    )
    return ratio, done, thick


def back_substitute(ratio, done):
    solved = list(done)
    for k in range(VERTICAL_LEVELS - 2, -1, -1):
        solved[k] = done[k] + ratio[k] * solved[k + 1]
    return solved


def shift(field, beside, amount):
    cols = field.shape[1] // 2
    lane = lax.broadcasted_iota(jnp.int32, (field.shape[0], cols), 1)
    crossing = lane == (0 if amount == 1 else cols - 1)
    turned = pltpu.roll(field[:, :cols], amount % cols, 1)
    return jnp.concatenate(
        [jnp.where(crossing, beside, turned), jnp.where(crossing, turned, beside)], axis=1
    )


def subcycle(moving, fixed, beside):
    u, v, s1, s2, s12 = moving
    strength, keep, push_scale, force_x, force_y = fixed
    rows, cols = u.shape[0], u.shape[1] // 2

    def lanes(f, amount):
        return pltpu.roll(f[:, cols:], amount % cols, 1)

    def dx(f, sides=None):
        sides = sides or (lanes(f, -1), lanes(f, 1))
        return shift(f, sides[0], -1) - shift(f, sides[1], 1)

    def dy(f):
        return pltpu.roll(f, rows - 1, 0) - pltpu.roll(f, 1, 0)

    ux, vy, uy, vx = dx(u, beside[0]), dy(v), dy(u), dx(v, beside[1])
    divergence = 0.5 * (ux + vy)
    tension = 0.5 * (ux - vy)
    shearing = 0.5 * (uy + vx)
    square = (
        divergence * divergence
        + (tension * tension + shearing * shearing) * (1.0 / ELLIPSE_SQUARE)
        + STRAIN_FLOOR
    )
    inverse = lax.rsqrt(square)
    deformation = square * inverse
    relax = 1.0 / (1.0 + STRESS_RELAX)
    viscous = (STRESS_RELAX * relax) * strength * inverse
    s1 = relax * s1 + viscous * (divergence - deformation)
    s2 = relax * s2 + viscous * tension * (1.0 / ELLIPSE_SQUARE)
    s12 = relax * s12 + viscous * shearing * (0.5 / ELLIPSE_SQUARE)
    push_x = dx(0.5 * (s1 + s2)) + dy(s12)
    push_y = dx(s12) + dy(0.5 * (s1 - s2))
    u = keep * u + push_scale * push_x + force_x
    v = keep * v + push_scale * push_y + force_y
    return u, v, s1, s2, s12


def as_column(row, rows):
    shape = (rows, rows)
    pick = lax.broadcasted_iota(jnp.int32, shape, 0) == lax.broadcasted_iota(jnp.int32, shape, 1)
    wide = jnp.broadcast_to(row.astype(jnp.float32), shape)
    return jnp.sum(jnp.where(pick, wide, 0.0), axis=1, keepdims=True)


def kernel(n_lat, n_lon, *refs):
    inputs, outputs, scratch = refs[:12], refs[12:17], refs[17:]
    temp_out, thick_out, vel_out, stress_out, zonal_out = outputs
    (held, strips, land_in, own, packed, edges, sides, parts, outbox) = scratch[:9]
    (in_sem, send_sem, recv_sem) = scratch[9:]
    rows, cols = land_in.shape
    devices = n_lat * n_lon
    lat, lon = lax.axis_index("lat"), lax.axis_index("lon")
    lats = [lax.rem(lat + d, n_lat) for d in range(n_lat)]
    lons = [lax.rem(lon + d, n_lon) for d in range(n_lon)]
    south, north, east, west = lats[1], lats[-1], lons[1], lons[-1]
    me = lon * n_lat + lat
    at_top, at_bottom = lat == 0, lat == n_lat - 1
    at_rim = at_top | at_bottom

    (temp_src, depth_src, area_src, surf_src, sea_src, vel_src, stress_src) = inputs[:7]
    (wind_src, current_src, land_src, ice_src, band_src) = inputs[7:]
    surf_in, sea_in = held.at[FAST], held.at[FAST + 1]
    depth_at = range(DEPTH_CLASSES)
    area_at = range(DEPTH_CLASSES, 2 * DEPTH_CLASSES)
    first_temp = FAST + 2
    temp_at = range(first_temp, first_temp + COLUMN_LAYERS)
    temp_loads, blocks = [], []
    layer = 0
    for group, count in enumerate(GROUPS):
        end = layer + count * VERTICAL_LEVELS
        begin = first_temp + layer if group else FAST
        blocks.append(held.at[pl.ds(begin, first_temp + end - begin)])
        temp_loads.append([])
        while layer < end:
            some = min(CHUNK, end - layer)
            temp_loads[group].append(
                (temp_src.at[pl.ds(layer, some)], held.at[pl.ds(first_temp + layer, some)], group)
            )
            layer += some
    start = 2 * DEPTH_CLASSES
    last = len(GROUPS) - 1
    vel_in, stress_in = held.at[pl.ds(start, 2)], held.at[pl.ds(start + 2, 3)]
    wind_in, current_in = held.at[pl.ds(start + 5, 2)], held.at[pl.ds(start + 7, 2)]
    fast_loads = [
        (vel_src, vel_in, last + 3),
        (stress_src, stress_in, last + 3),
        (wind_src, wind_in, last + 3),
        (current_src, current_in, last + 3),
        (land_src, land_in, last + 2),
    ]
    loads = [
        *fast_loads,
        (depth_src, held.at[pl.ds(0, DEPTH_CLASSES)], last + 3),
        (area_src, held.at[pl.ds(DEPTH_CLASSES, DEPTH_CLASSES)], last + 3),
        (surf_src, surf_in, 0),
        (sea_src, sea_in, 0),
        *temp_loads[0],
        (band_src, strips.at[0], last + 1),
        (ice_src, strips.at[1], last + 1),
        *[load for group in temp_loads[1:] for load in group],
    ]
    for source, target, group in loads:
        pltpu.make_async_copy(source, target, in_sem.at[group]).start()

    def arrive(ref, semaphore):
        pltpu.make_async_copy(ref, ref, semaphore).wait()

    def arrive_planes(inner, rim, semaphore):
        @pl.when(at_rim)
        def _():
            arrive(held.at[pl.ds(0, rim)], semaphore)

        @pl.when(jnp.logical_not(at_rim))
        def _():
            arrive(held.at[pl.ds(0, inner)], semaphore)

    pairs = [(a, g) for g in lons[1:] for a in lats[n_lat // 2 :] + lats[: n_lat // 2]] + [(a, lon) for a in lats[1:]]

    def everyone(visit):
        def step(d, carry):
            other = lax.rem(me + 1 + d, devices)
            visit((lax.rem(other, n_lat), other // n_lat))
            return carry

        lax.fori_loop(0, devices - 1, step, 0)

    barrier = pltpu.get_barrier_semaphore()

    def greet(device):
        pl.semaphore_signal(barrier, inc=1, device_id=device, device_id_type=MESH)

    if devices <= UNROLLED:
        for pair in pairs[1 - n_lat :] + pairs[: 1 - n_lat]:
            greet(pair)
    else:
        everyone(greet)

    kept = []

    def thermo(c):
        temps = [held[temp_at[c * VERTICAL_LEVELS + k]] for k in range(VERTICAL_LEVELS)]
        depth = held[depth_at[c]]
        ratio, done, thick = step_columns(temps, depth, surf_in[...], sea_in[...])
        kept.append((ratio, done, thick))

    def finish_temps(c):
        for k, solved in enumerate(back_substitute(*kept[c][:2])):
            temp = held[temp_at[c * VERTICAL_LEVELS + k]]
            temp_out[c * VERTICAL_LEVELS + k] = jnp.where(icy, solved, temp)

    def send_part(device):
        pltpu.make_async_remote_copy(
            src_ref=outbox.at[pl.ds(2 * device[0], 2)],
            dst_ref=parts.at[pl.ds(2 * me, 2)],
            send_sem=send_sem.at[0],
            recv_sem=recv_sem.at[0],
            device_id=device,
            device_id_type=MESH,
        ).start()

    def send_halo(source, target, device, arrival):
        pltpu.make_async_remote_copy(
            src_ref=source,
            dst_ref=target,
            send_sem=send_sem.at[1],
            recv_sem=recv_sem.at[arrival],
            device_id=device,
            device_id_type=MESH,
        ).start()

    arrive(held.at[pl.ds(0, FAST)], in_sem.at[last + 3])
    arrive(land_in, in_sem.at[last + 2])
    volume = held[area_at[0]] * held[depth_at[0]]
    coverage = held[area_at[0]]
    for c in range(1, DEPTH_CLASSES):
        volume = volume + held[area_at[c]] * held[depth_at[c]]
        coverage = coverage + held[area_at[c]]
    strength = volume * jnp.exp(-STRENGTH_DECAY * (1.0 - coverage))
    drag = 1.0 / (1.0 + MOMENTUM_STEP * WATER_DRAG)
    keep = land_in[...].astype(jnp.float32) * drag
    forced = MOMENTUM_STEP * keep
    push_scale = 0.5 * forced / (1.0 + volume)
    fields = [vel_in[0], vel_in[1], stress_in[0], stress_in[1], stress_in[2], strength, keep]
    fields += [push_scale]
    fields += [forced * (wind_in[i] + WATER_DRAG * current_in[i]) for i in range(2)]
    lane = lax.broadcasted_iota(jnp.int32, (rows, cols), 1)
    pack = jnp.zeros((rows, cols), jnp.float32)
    for f in range(FIELDS):
        first = 2 * HALO * f
        turned = pltpu.roll(fields[f], (first + HALO) % cols, 1)
        pack = jnp.where((lane >= first) & (lane < first + 2 * HALO), turned, pack)
    packed[...] = pack
    for f in range(FIELDS):
        own[f] = fields[f]

    arrive(blocks[0], in_sem.at[0])
    for c in range(0, 2):
        thermo(c)
    pl.semaphore_wait(barrier, devices - 1)

    tail, head = pl.ds(rows - EDGE, EDGE), pl.ds(0, EDGE)
    above, middle, below = pl.ds(0, EDGE), pl.ds(EDGE, rows), pl.ds(EDGE + rows, EDGE)
    send_halo(packed, sides.at[0, middle], (lat, east), 1)
    send_halo(packed, sides.at[1, middle], (lat, west), 1)

    @pl.when(jnp.logical_not(at_bottom))
    def _():
        send_halo(packed.at[tail], sides.at[0, above], (south, east), 1)
        send_halo(packed.at[tail], sides.at[1, above], (south, west), 1)
        for kind, reach in EDGE_KINDS:
            send_halo(
                own.at[kind, pl.ds(rows - reach, reach)],
                edges.at[0, kind, pl.ds(EDGE - reach, reach)],
                (south, lon),
                2,
            )

    @pl.when(jnp.logical_not(at_top))
    def _():
        send_halo(packed.at[head], sides.at[0, below], (north, east), 1)
        send_halo(packed.at[head], sides.at[1, below], (north, west), 1)
        for kind, reach in EDGE_KINDS:
            send_halo(
                own.at[kind, pl.ds(0, reach)],
                edges.at[1, kind, pl.ds(0, reach)],
                (north, lon),
                2,
            )

    arrive(blocks[1], in_sem.at[1])
    arrive(strips, in_sem.at[last + 1])
    icy = as_column(strips[1], rows) == 1.0
    band = as_column(strips[0], rows).astype(jnp.int32)
    slot = lax.broadcasted_iota(jnp.int32, (rows, cols), 1)
    slot = jnp.where(slot < BANDS_DEV, slot, -BANDS_DEV * n_lat)
    members = [band - BANDS_DEV * a == slot for a in range(n_lat)]
    for a in range(n_lat):
        counted = jnp.where(members[a], float(cols), 0.0)
        outbox[pl.ds(2 * a + 1, 1)] = jnp.sum(counted, axis=0, keepdims=True)

    for c in range(2, 5):
        thermo(c)
    after = jnp.zeros((rows, cols), jnp.float32)
    for c in range(DEPTH_CLASSES):
        thick = jnp.where(icy, kept[c][2], held[depth_at[c]])
        thick_out[c] = thick
        after = after + held[area_at[c]] * thick
    total = jnp.sum(after, axis=1, keepdims=True)
    for a in range(n_lat):
        outbox[pl.ds(2 * a, 1)] = jnp.sum(jnp.where(members[a], total, 0.0), axis=0, keepdims=True)
    if devices <= UNROLLED:
        for pair in pairs[0:]:
            send_part(pair)
    else:
        everyone(send_part)

    for c in range(DEPTH_CLASSES):
        finish_temps(c)

    parts[pl.ds(2 * me, 2)] = outbox[pl.ds(2 * lat, 2)]

    def finish_zonal():
        whole = jnp.sum(parts[...].reshape(-1, 8, cols), axis=0)
        whole = whole + pltpu.roll(whole, 4, 0)
        whole = whole + pltpu.roll(whole, 2, 0)
        mean = whole[:1] / jnp.maximum(whole[1:2], 1.0)
        zonal_out[...] = mean[:, :BANDS_DEV]

    brim = EDGE_ROWS // rows
    arrive_planes(2 * brim, brim, recv_sem.at[2])
    arrive_planes(4, 3, recv_sem.at[1])
    tall = rows + 2 * EDGE
    low = jnp.where(at_top, EDGE, 0)
    high = jnp.where(at_bottom, EDGE + rows, tall)
    row_id = lax.broadcasted_iota(jnp.int32, (tall, cols), 0)
    inside = (row_id >= low) & (row_id < high)
    place = lax.broadcasted_iota(jnp.int32, (tall, cols), 1)
    merged = jnp.where(lax.rem(place, 2 * HALO) < HALO, sides[0], sides[1])
    merged = jnp.where(inside, merged, 0.0)

    def beside(f, amount):
        return pltpu.roll(merged, (2 * cols - 2 * HALO * f - HALO + amount) % cols, 1)

    state = []
    for f in range(FIELDS):
        centre = jnp.concatenate([edges[0, f], own[f], edges[1, f]], axis=0)
        centre = jnp.where(inside, centre, 0.0)
        state.append(jnp.concatenate([centre, beside(f, 0)], axis=1))
    moving, fixed = state[:5], state[5:]
    first_beside = [(beside(f, -1), beside(f, 1)) for f in range(2)]
    others = parts.at[pl.ds(0, 2 * (devices - 1))]
    for turn in range(SUBCYCLES):
        if turn == PARTS_TURN:
            arrive(others, recv_sem.at[0])
            finish_zonal()
        moving = subcycle(moving, fixed, first_beside if turn == 0 else (None, None))
    for i in range(2):
        vel_out[i] = moving[i][EDGE : EDGE + rows, :cols]
    for i in range(3):
        stress_out[i] = moving[2 + i][EDGE : EDGE + rows, :cols]

    arrive_planes(2 + 2 * (brim + 1), 2 + brim + 1, send_sem.at[1])
    arrive(others, send_sem.at[0])
    if PARTS_TURN == SUBCYCLES:
        arrive(others, recv_sem.at[0])
        finish_zonal()


def put_out(temp, thick, vel, stress, zonal, *refs):
    outs, sem = refs[:5], refs[5]
    planes = [ref.shape[0] for ref in (thick, vel, stress)]
    copies = [(zonal, outs[4], 2), (vel, outs[2], 1), (stress, outs[3], 1), (thick, outs[1], 1)]
    for first in range(0, COLUMN_LAYERS, OUT_CHUNK):
        some = pl.ds(first, min(OUT_CHUNK, COLUMN_LAYERS - first))
        copies.append((temp.at[some], outs[0].at[some], 0))
    for source, target, group in copies:
        pltpu.make_async_copy(source, target, sem.at[group]).start()
    pltpu.make_async_copy(temp, outs[0], sem.at[0]).wait()
    small = pl.ds(0, sum(planes))
    pltpu.make_async_copy(temp.at[small], outs[0].at[small], sem.at[1]).wait()
    pltpu.make_async_copy(zonal, outs[4], sem.at[2]).wait()


def local(n_lat, n_lon, *args):
    args = list(args)
    args[:3] = [jnp.transpose(a, (1, 0, 2)) for a in args[:3]]
    args[11] = args[11].reshape(1, -1)
    rows, cols = args[3].shape
    tall = rows + 2 * EDGE
    f32 = jnp.float32
    vmem = pl.BlockSpec(memory_space=pltpu.VMEM)
    shapes = [args[i].shape for i in (0, 1, 5, 6)] + [(1, BANDS_DEV)]
    dma = pltpu.SemaphoreType.DMA
    results = pl.pallas_call(
        functools.partial(kernel, n_lat, n_lon),
        out_shape=[pltpu.VMEM(shape, f32) for shape in shapes],
        in_specs=[pl.BlockSpec(memory_space=pl.ANY)] * 12,
        out_specs=[vmem] * 5,
        scratch_shapes=[
            pltpu.VMEM((2 * DEPTH_CLASSES + 2 + COLUMN_LAYERS + 9, rows, cols), f32),
            pltpu.VMEM((2, 1, rows), jnp.int32),
            pltpu.VMEM((rows, cols), jnp.int32),
            pltpu.VMEM((FIELDS, rows, cols), f32),
            pltpu.VMEM((rows, cols), f32),
            pltpu.VMEM((2, FIELDS, EDGE, cols), f32),
            pltpu.VMEM((2, tall, cols), f32),
            pltpu.VMEM((2 * n_lat * n_lon, cols), f32),
            pltpu.VMEM((2 * n_lat, cols), f32),
            dma((len(GROUPS) + 3,)),
            dma((2,)),
            dma((3,)),
        ],
        compiler_params=pltpu.CompilerParams(collective_id=0, has_side_effects=True),
        name="ice_step",
    )(*args)
    temp, thick, vel, stress, zonal = pl.pallas_call(
        put_out,
        out_shape=[jax.ShapeDtypeStruct(shape, f32) for shape in shapes],
        in_specs=[vmem] * 5,
        out_specs=[pl.BlockSpec(memory_space=pl.ANY)] * 5,
        scratch_shapes=[dma((3,))],
        name="put_out",
    )(*[pltpu.with_memory_space_constraint(r, pltpu.VMEM) for r in results])
    temp, thick = [jnp.transpose(a, (1, 0, 2)) for a in (temp, thick)]
    return (temp, thick, vel, stress, zonal.reshape(BANDS_DEV))


def solution(mesh):
    shape = dict(mesh.shape)
    return jax.shard_map(
        functools.partial(local, shape["lat"], shape["lon"]),
        mesh=mesh,
        in_specs=(
            P("lat", None, "lon"),
            P("lat", None, "lon"),
            P("lat", None, "lon"),
            P("lat", "lon"),
            P("lat", "lon"),
            P(None, "lat", "lon"),
            P(None, "lat", "lon"),
            P(None, "lat", "lon"),
            P(None, "lat", "lon"),
            P("lat", "lon"),
            P("lon", "lat"),
            P("lat"),
        ),
        out_specs=(
            P("lat", None, "lon"),
            P("lat", None, "lon"),
            P(None, "lat", "lon"),
            P(None, "lat", "lon"),
            P("lat"),
        ),
        check_vma=False,
    )
```
